32 devices in a mesh: row: 16 (over z, y, x), col: 2 (over core).
Axes of the slice: x: 2, y: 2, z: 4, core: 2. Of those that a mesh axis runs over, the one named last changes fastest.
Arguments:
- new_aux: bfloat16 [2048, 4096], P('row', 'col'), may hold values from -6 to 6
- former_auxiliary_rows: bfloat16 [20480, 4096], P('row', 'col'), may hold values from -6 to 6
- old_emb: bfloat16 [20480, 4096], P('row', 'col'), may hold values from -6 to 6
- neighbour_ids: int32 [2048, 16], P('row'), may hold values from -1 to 20479, as said below
- neighbour_counts: int32 [2048], P('row'), may hold values from 8 to 16
Outputs:
- new_emb: bfloat16 [2048, 4096], P('row', 'col')
The draws below stay inside these ranges and needn't reach their ends.
Inputs may be any that keep to these rules, and one draw needn't show every extreme that they name: neighbour_ids[j, k] is an old row number for k < neighbour_counts[j] and -1 otherwise. The live entries of the 128 new rows of one index of row name at most 192 entries, and at most 96 different rows, within one block of 1280 old rows held by one index of row; both bounds are reached in every draw.
All inputs are finite; a program needn't handle non-finite values.
Results may differ from the reference program's by a relative error of at most 0.0049.
Values may be sent and summed in bfloat16 or wider, within the bound.
No kernel may reach another device: no remote copies, remote signals or barrier semaphores. Data moves between devices by JAX's collectives and lax.ppermute only.
A program may use at most 128 MiB of HBM per device.

```python
import jax
import jax.numpy as jnp
from jax import lax

D = 4096
OLD_DEV = 1280
NEW_DEV = 128
NEIGHBOURS = 16
OLD_ROWS = 20480
FRESH_ROW_COUNT = 2048
CAPACITY = 192
DISTINCT = 96
N_ROW = 16


def adjacent_lookup_lists(key):
    counts = jax.random.randint(jax.random.fold_in(key, 11), (FRESH_ROW_COUNT,), 8, NEIGHBOURS + 1).astype(jnp.int32)
    admissible_flags = jnp.arange(NEIGHBOURS, dtype=jnp.int32)[None, :] < counts[:, None]
    live_blocks = admissible_flags.reshape(N_ROW, NEW_DEV * NEIGHBOURS)
    ranks = jnp.cumsum(live_blocks.astype(jnp.int32), axis=1) - 1
    total = N_ROW * CAPACITY
    sharpest_weighting = jax.random.randint(jax.random.fold_in(key, 12), (), 0, N_ROW).astype(jnp.int32)
    order_keys = jax.random.split(jax.random.fold_in(key, 13), N_ROW)
    positions = jax.vmap(lambda k: jax.random.permutation(k, total))(order_keys).astype(jnp.int32)
    slot_owner = jnp.arange(total, dtype=jnp.int32) // CAPACITY
    priority = jnp.where(slot_owner == sharpest_weighting, 0, total)[None, :].astype(jnp.int32) + positions
    order = jnp.argsort(priority, axis=1).astype(jnp.int32)
    slots = jnp.take_along_axis(order, jnp.clip(ranks, 0, total - 1), axis=1)
    owners = slots // CAPACITY
    within = slots % CAPACITY % DISTINCT
    pool_keys = jax.random.split(jax.random.fold_in(key, 14), N_ROW * N_ROW)
    pools = jax.vmap(lambda k: jax.random.permutation(k, OLD_DEV)[:DISTINCT])(pool_keys).astype(jnp.int32)
    pools = pools.reshape(N_ROW, N_ROW, DISTINCT)
    block_index = jnp.arange(N_ROW, dtype=jnp.int32)[:, None]
    local_rows = pools[block_index, owners, within]
    numbers = owners * OLD_DEV + local_rows
    numbers = jnp.where(live_blocks, numbers, -1).reshape(FRESH_ROW_COUNT, NEIGHBOURS).astype(jnp.int32)
    return (numbers, counts)


def draw_neighbour_ids(key, part):
    return adjacent_lookup_lists(key)[0]


def draw_neighbour_counts(key, part):
    return adjacent_lookup_lists(key)[1]


def level_of(own_key, dims, shards, smallest, high):
    def one(dim, parts):
        draws = jax.random.uniform(jax.random.fold_in(jax.random.fold_in(own_key, 6), dim), (parts,), jnp.float32, smallest / len(shards), high / len(shards))
        return jnp.repeat(jnp.exp(draws), dims[dim] // parts).reshape((-1,) + (1,) * (len(dims) - dim - 1))

    loudness = one(*shards[0])
    for cut in shards[1:]:
        loudness = loudness * one(*cut)
    return loudness


def gaussian(stream_key, dims, spread, bound, cuts=(), held_as=jnp.bfloat16):
    result = spread * jax.random.normal(stream_key, dims, jnp.float32)
    if cuts:
        result = result * level_of(stream_key, dims, cuts, -0.22, 0.18)
    return jnp.clip(result, -bound, bound).astype(held_as)


def setup_inputs(seed: int = 0) -> dict:
    keys = jax.random.split(jax.random.key(seed), 6)
    return {
        "new_aux": gaussian(keys[0], (FRESH_ROW_COUNT, D), 1.0, 6.0, ((0, 16), (1, 2))),
        "former_auxiliary_rows": gaussian(keys[1], (OLD_ROWS, D), 1.0, 6.0, ((0, 16), (1, 2))),
        "old_emb": gaussian(keys[2], (OLD_ROWS, D), 1.0, 6.0, ((0, 16), (1, 2))),
        "neighbour_ids": draw_neighbour_ids(jax.random.fold_in(keys[5], 71), 0),
        "neighbour_counts": draw_neighbour_counts(jax.random.fold_in(keys[5], 71), 0),
    }


eps = 1e-06
exponential_sharpness = 0.025

def blend_block(args):
    former_auxiliary_rows, old_emb, aux_block, neighbour_index_block, admissible_flag_tile = args
    near_aux = former_auxiliary_rows[neighbour_index_block].astype(jnp.float32)
    near_emb = old_emb[neighbour_index_block].astype(jnp.float32)
    own = aux_block.astype(jnp.float32)
    inner = jnp.einsum('jd,jkd->jk', own, near_aux)
    near_sq = jnp.einsum('jkd,jkd->jk', near_aux, near_aux)
    own_sq = jnp.einsum('jd,jd->j', own, own)
    angular_similarity_values = inner * lax.rsqrt((own_sq[:, None] + eps) * (near_sq + eps))
    plain_affinity_values = jnp.where(admissible_flag_tile, jnp.exp(angular_similarity_values / exponential_sharpness), jnp.float32(0.0))
    weights = (plain_affinity_values / lax.optimization_barrier(jnp.sum(plain_affinity_values, axis=1, keepdims=True))).astype(jnp.bfloat16)
    blended = jnp.einsum('jk,jkd->jd', weights.astype(jnp.float32), near_emb)
    return blended.astype(jnp.bfloat16)

def reference(new_aux, former_auxiliary_rows, old_emb, neighbour_ids, neighbour_counts):
    admissible_flags = jnp.arange(NEIGHBOURS, dtype=jnp.int32)[None, :] < neighbour_counts[:, None]
    safe = jnp.where(admissible_flags, neighbour_ids, 0).astype(jnp.int32)

    def one(args):
        aux_block, neighbour_index_block, admissible_flag_tile = args
        return blend_block((former_auxiliary_rows, old_emb, aux_block, neighbour_index_block, admissible_flag_tile))
    blocks = lax.map(one, (new_aux.reshape(N_ROW, NEW_DEV, D), safe.reshape(N_ROW, NEW_DEV, NEIGHBOURS), admissible_flags.reshape(N_ROW, NEW_DEV, NEIGHBOURS)))
    return blocks.reshape(FRESH_ROW_COUNT, D)
```

```python
import functools

import jax
import jax.numpy as jnp
from jax import lax
from jax.experimental import pallas as pl
from jax.experimental.pallas import tpu as pltpu
from jax.sharding import PartitionSpec as P

eps = 1e-06
exponential_sharpness = 0.025


def exchange_local(new_aux, former_auxiliary_rows, old_emb, neighbour_ids, neighbour_counts):
    devices = lax.axis_size("row")
    old_dev = former_auxiliary_rows.shape[0]
    new_dev, slots_row = neighbour_ids.shape
    width = new_aux.shape[1]
    capacity = 24 * new_dev // devices
    admissible_flags = jnp.arange(slots_row, dtype=jnp.int32)[None, :] < neighbour_counts[:, None]
    flat_ids = neighbour_ids.reshape(-1)
    flat_live = admissible_flags.reshape(-1)
    owners = jnp.where(flat_live, flat_ids // old_dev, devices)
    local_rows = jnp.where(flat_live, flat_ids - owners * old_dev, 0)
    onehot = (owners[:, None] == jnp.arange(devices, dtype=jnp.int32)[None, :]).astype(jnp.int32)
    ranks = jnp.sum(onehot * (jnp.cumsum(onehot, axis=0) - 1), axis=1)
    slots = jnp.where(flat_live, owners * capacity + ranks, devices * capacity)
    requests = jnp.full((devices * capacity + 1,), -1, jnp.int32).at[slots].set(local_rows)
    requests = requests[:-1].reshape(devices, capacity)
    clipped_owner = jnp.clip(owners, 0, devices - 1)
    distinct = capacity // 2
    sorted_sequence = jnp.sort(requests, axis=1)
    previous = jnp.concatenate(
        [jnp.full((devices, 1), -1, jnp.int32), sorted_sequence[:, :-1]], axis=1
    )
    first = (sorted_sequence >= 0) & (sorted_sequence != previous)
    position = jnp.cumsum(first.astype(jnp.int32), axis=1) - 1
    target = jnp.where(first, position, distinct)
    compact = jnp.full((devices, distinct + 1), -1, jnp.int32)
    compact = compact.at[jnp.arange(devices, dtype=jnp.int32)[:, None], target].set(
        sorted_sequence
    )[:, :distinct]
    candidates = compact[clipped_owner]
    matches = (candidates == local_rows[:, None]).astype(jnp.int32)
    found = jnp.sum(matches * jnp.arange(distinct, dtype=jnp.int32)[None, :], axis=1)
    entry_slot = clipped_owner * distinct + found
    safe = jnp.clip(
        lax.all_to_all(compact, "row", split_axis=0, concat_axis=0, tiled=True), 0, old_dev - 1
    )
    aux_rows = jnp.take(former_auxiliary_rows, safe, axis=0)
    emb_rows = jnp.take(old_emb, safe, axis=0)
    aux_back = lax.all_to_all(aux_rows, "row", split_axis=0, concat_axis=0, tiled=True)
    emb_back = lax.all_to_all(emb_rows, "row", split_axis=0, concat_axis=0, tiled=True)
    near_aux = jnp.take(aux_back.reshape(-1, width), entry_slot, axis=0).reshape(
        new_dev, slots_row, width
    )
    near_emb = jnp.take(emb_back.reshape(-1, width), entry_slot, axis=0).reshape(
        new_dev, slots_row, width
    )
    inner = jnp.einsum("jd,jkd->jk", new_aux, near_aux, preferred_element_type=jnp.float32)
    near_sq = jnp.einsum("jkd,jkd->jk", near_aux, near_aux, preferred_element_type=jnp.float32)
    own_sq = jnp.einsum("jd,jd->j", new_aux, new_aux, preferred_element_type=jnp.float32)
    inner, near_sq, own_sq = lax.psum((inner, near_sq, own_sq), "col")
    angular_similarity_values = inner * lax.rsqrt((own_sq[:, None] + eps) * (near_sq + eps))
    plain_affinity_values = jnp.where(
        admissible_flags,
        jnp.exp(angular_similarity_values / exponential_sharpness),
        jnp.float32(0.0),
    )
    weights = (
        plain_affinity_values / jnp.sum(plain_affinity_values, axis=1, keepdims=True)
    ).astype(jnp.bfloat16)
    blended = jnp.einsum("jk,jkd->jd", weights, near_emb, preferred_element_type=jnp.float32)
    return blended.astype(jnp.bfloat16)


def count_kernel(base_ref, small_ref, out_ref):
    slots = small_ref.shape[1] - 8
    new_dev, old_dev = out_ref.shape[1:]
    lanes = 128
    chunks = old_dev // lanes
    per_word = 6
    words = -(-chunks // per_word)
    base = base_ref[0]
    ids = small_ref[0].T[:, :slots].astype(jnp.int32) - base
    inside = (ids >= 0) & (ids < old_dev)
    low = ids & (lanes - 1)
    chunk = ids >> 7
    adds = []
    for w in range(words):
        here = inside & (chunk >= w * per_word) & (chunk < (w + 1) * per_word)
        shift = jnp.where(here, (chunk - w * per_word) * 5, 0)
        adds.append(jnp.where(here, jnp.left_shift(1, shift), 0))
    iota = lax.broadcasted_iota(jnp.int32, (new_dev, lanes), 1)
    acc = [jnp.zeros((new_dev, lanes), jnp.int32) for _ in range(words)]
    for k in range(slots):
        match = low[:, k : k + 1] == iota
        for w in range(words):
            acc[w] = acc[w] + jnp.where(match, adds[w][:, k : k + 1], 0)
    for c in range(chunks):
        bits = (acc[c // per_word] >> (5 * (c % per_word))) & 31
        out_ref[0, :, c * lanes : (c + 1) * lanes] = bits.astype(jnp.float32).astype(jnp.bfloat16)


def count_of(small, base, old_dev, slots):
    blocks, rows, new_dev = small.shape
    return pl.pallas_call(
        count_kernel,
        grid=(blocks,),
        in_specs=[
            pl.BlockSpec(memory_space=pltpu.SMEM),
            pl.BlockSpec((1, rows, new_dev), lambda b: (b, 0, 0)),
        ],
        out_specs=pl.BlockSpec((1, new_dev, old_dev), lambda b: (b, 0, 0)),
        out_shape=jax.ShapeDtypeStruct((blocks, new_dev, old_dev), jnp.bfloat16),
        cost_estimate=pl.CostEstimate(
            flops=blocks * new_dev * 128 * slots * 60,
            bytes_accessed=blocks * new_dev * old_dev * 2,
            transcendentals=0,
        ),
        name="count",
    )(base, small)


def dot_nt(a, b):
    return lax.dot_general(a, b, (((1,), (1,)), ((), ())), preferred_element_type=jnp.float32)


def dot_nn(a, b):
    return lax.dot_general(a, b, (((1,), (0,)), ((), ())), preferred_element_type=jnp.float32)


def meet_local(new_aux, former, old_emb, neighbour_ids, neighbour_counts):
    devices = lax.axis_size("row")
    depth = devices // 4
    old_dev = former.shape[0]
    new_dev, slots = neighbour_ids.shape

    def perm(f):
        out = []
        for z in range(depth):
            for y in range(2):
                for x in range(2):
                    a, b, c = f(z, y, x)
                    out.append(((z * 2 + y) * 2 + x, (a % depth * 2 + b) * 2 + c))
        return out

    def over_x(v):
        return lax.ppermute(v, "row", perm(lambda z, y, x: (z, y, 1 - x)))

    def over_y(v):
        return lax.ppermute(v, "row", perm(lambda z, y, x: (z, 1 - y, x)))

    def over_z(v, k):
        return lax.ppermute(v, "row", perm(lambda z, y, x: (z + k, y, x)))

    def over_col(v):
        return lax.ppermute(v, "col", [(0, 1), (1, 0)])

    order = sorted(range(1, depth), key=lambda k: min(k, depth - k))
    f32 = jnp.float32
    own_half = jnp.sum(jnp.square(new_aux.astype(f32)), axis=1)
    near_half = jnp.sum(jnp.square(former.astype(f32)), axis=1)
    halves = jnp.concatenate([own_half, near_half])
    squares = halves + over_col(halves)
    own_scale = lax.rsqrt(squares[:new_dev] + eps)
    near_scale = lax.rsqrt(squares[new_dev:] + eps) * f32(1.0 / exponential_sharpness)

    column = {0: new_aux}
    for k in order:
        column[k] = over_z(new_aux, k)
    blocks = {}
    for k in [0] + order:
        o = column[k]
        blocks[k, 0, 0] = o
        if k % 2 == 0:
            p = over_y(o)
            blocks[k, 1, 0] = p
            blocks[k, 0, 1] = over_x(o)
            blocks[k, 1, 1] = over_x(p)
        else:
            p = over_x(o)
            blocks[k, 0, 1] = p
            blocks[k, 1, 0] = over_y(o)
            blocks[k, 1, 1] = over_y(p)

    live = jnp.arange(slots, dtype=jnp.int32)[None, :] < neighbour_counts[:, None]
    ids = jnp.where(live, neighbour_ids, -1).astype(f32).T
    small = jnp.concatenate([ids, jnp.broadcast_to(own_scale[None, :], (8, new_dev))])
    small = jnp.stack([small] + [over_z(small, k) for k in range(1, depth)])
    small = jnp.concatenate([small, over_y(small)])
    small = jnp.concatenate([small, over_x(small)])
    base = jnp.full((1,), lax.axis_index("row") * old_dev, jnp.int32)
    counts = count_of(small, base, old_dev, slots)
    scales = small[:, slots, :]

    def slot_of(k, y, x):
        return (x * 2 + y) * depth + k

    raw, total = {}, {}
    for k in [0] + order:
        keys = [(k, y, x) for y in range(2) for x in range(2)]
        half = jnp.concatenate([dot_nt(blocks[key], former) for key in keys])
        inner = half + over_col(half)
        here = [slot_of(*key) for key in keys]
        scale = jnp.concatenate([scales[s] for s in here])
        count = jnp.concatenate([counts[s] for s in here]).astype(f32)
        value = count * jnp.exp(inner * (scale[:, None] * near_scale[None, :]))
        sums = jnp.sum(value, axis=1).reshape(4, new_dev)
        value = value.astype(jnp.bfloat16).reshape(4, new_dev, old_dev)
        for i, key in enumerate(keys):
            raw[key] = value[i]
            total[slot_of(*key)] = sums[i]

    totals = jnp.stack([total[s] for s in range(devices)])
    half_way = devices // 2
    totals = totals[:half_way] + over_x(totals[half_way:])
    totals = totals[:depth] + over_y(totals[depth:])
    denominator = totals[0]
    for k in range(1, depth):
        denominator = denominator + over_z(totals[k], -k)

    def part(key):
        return dot_nn(raw[key], old_emb)

    def narrow(v):
        return v.astype(jnp.bfloat16)

    back = {}
    for k in order + [0]:
        if k % 2 == 0:
            far, mid, near = over_x, over_y, (k, 0, 1)
            middle = (k, 1, 0)
        else:
            far, mid, near = over_y, over_x, (k, 1, 0)
            middle = (k, 0, 1)
        first = far(narrow(part((k, 1, 1))))
        second = far(narrow(part(near)))
        third = mid(narrow(part(middle) + first.astype(f32)))
        whole = part((k, 0, 0)) + second.astype(f32) + third.astype(f32)
        back[k] = whole if k == 0 else over_z(narrow(whole), -k)
    blend = back[0]
    for k in order:
        blend = blend + back[k].astype(f32)
    return (blend / denominator[:, None]).astype(jnp.bfloat16)


def solution(mesh):
    fits = mesh.shape["col"] == 2 and mesh.shape["row"] % 4 == 0
    return jax.shard_map(
        meet_local if fits else exchange_local,
        mesh=mesh,
        in_specs=(P("row", "col"), P("row", "col"), P("row", "col"), P("row", None), P("row")),
        out_specs=P("row", "col"),
        check_vma=False,
    )
```
